256 devices in a mesh: fit: 64 (over x, y_lo, z), col: 4 (over y_hi, core).
Axes of the slice: x: 4, y: 4 (y_hi: 2, y_lo: 2; y = y_hi * 2 + y_lo), z: 8, core: 2. Of those that a mesh axis runs over, the one named last changes fastest.
Arguments:
- trial: bfloat16 [8, 256, 512], P(None, 'fit', 'col'), may hold values from -6 to 6
- hole_factor: bfloat16 [2048, 256, 256], P('fit'), may hold values from -0.0234375 to 0.0234375
- elec_factor: bfloat16 [2048, 512, 512], P('fit', 'col'), may hold values from -0.25 to 0.25
- hole_energy: float32 [256], P('fit'), may hold values from -1.2 to -0.3
- elec_energy: float32 [512], P('col'), may hold values from 0.1 to 1.5
Outputs:
- applied: float32 [8, 256, 512], P(None, 'fit', 'col')
The draws below stay inside these ranges and needn't reach their ends.
All inputs are finite; a program needn't handle non-finite values.
Results may differ from the reference program's by a relative error of at most 0.0018.
Values may be sent and summed in bfloat16 or wider, within the bound.
A program may use at most 64 MiB of HBM per device.

```python
import jax
import jax.numpy as jnp
from jax import lax

O = 256
V = 512
AUX_DEV = 32
NVEC = 8
NAUX = 2048


def raised(drawn, rng, source, target, parts, factor):
    owner, partner = [(jnp.arange(drawn.shape[axis_at]) // (drawn.shape[axis_at] // parts)).reshape([-1 if axis == axis_at else 1 for axis in range(drawn.ndim)]) for axis_at in (source, target)]
    chosen = jax.random.permutation(rng, parts)[partner]
    strong = (owner == chosen) | (owner == (partner + parts // 2) % parts)
    return jnp.where(strong, factor * drawn, drawn)


def block_scale(own_key, extent, split, smallest, high):
    gain, own = 1.0, jax.random.fold_in(own_key, 6)
    for position, parts in split:
        steps = jnp.exp(jax.random.uniform(jax.random.fold_in(own, position), (parts,), jnp.float32, smallest / len(split), high / len(split)))
        gain = gain * jnp.repeat(steps, extent[position] // parts).reshape([-1 if axis == position else 1 for axis in range(len(extent))])
    return gain


def bell_draw(rng, shape, width, reach, split=(), dtype=jnp.bfloat16):
    drawn = jax.random.normal(rng, shape, jnp.float32) * width
    if len(split) > 0:
        drawn = block_scale(rng, shape, split, -0.22, 0.18) * drawn
    return jnp.clip(drawn, min=-reach, max=reach).astype(dtype)


def bell_draw_with(own_key, dims, scale, reach, cuts, heavy, held_as=jnp.bfloat16):
    array = scale * jax.random.normal(own_key, dims, jnp.float32)
    if cuts:
        array = array * block_scale(own_key, dims, cuts, -0.22, 0.18)
    return jnp.clip(raised(array, jax.random.fold_in(own_key, 3), *heavy), -reach, reach).astype(held_as)


def setup_inputs(seed: int = 0) -> dict:
    splits = jax.random.split(jax.random.key(seed), 6)
    return {
        "trial": bell_draw(splits[0], (NVEC, O, V), 1.0, 6.0, ((1, 64), (2, 4))),
        "hole_factor": bell_draw_with(splits[1], (NAUX, O, O), (O * NAUX) ** -0.5, 0.0234375, ((0, 64),), (0, 1, 64, 4.0)),
        "elec_factor": bell_draw(splits[2], (NAUX, V, V), V ** -0.5, 0.25, ((0, 64), (1, 4))),
        "hole_energy": jnp.clip(-1.2 + 0.90000004 * jax.random.uniform(splits[3], (O,), jnp.float32) ** block_scale(splits[3], (O,), ((0, 64),), -0.2, 0.2), -1.2, -0.3),
        "elec_energy": jnp.clip(0.1 + 1.4 * jax.random.uniform(splits[4], (V,), jnp.float32) ** block_scale(splits[4], (V,), ((0, 4),), -0.2, 0.2), 0.1, 1.5),
    }


def reference(trial, hole_factor, elec_factor, hole_energy, elec_energy):
    block = 64 if NAUX % 64 == 0 else AUX_DEV
    count = NAUX // block
    hole_blocks = hole_factor.reshape(count, block, O, O)
    elec_blocks = elec_factor.reshape(count, block, V, V)
    trial_wide = trial.astype(jnp.float32)

    def step(total, pieces):
        hole_part, elec_part = pieces
        half = jnp.einsum("kjb,pab->kpja", trial_wide, elec_part.astype(jnp.float32)).astype(jnp.bfloat16)
        total = total + jnp.einsum("pij,kpja->kia", hole_part.astype(jnp.float32), half.astype(jnp.float32))
        return total, None

    direct, _ = lax.scan(step, jnp.zeros((NVEC, O, V), jnp.float32), (hole_blocks, elec_blocks))
    spread = elec_energy[None, :] - hole_energy[:, None]
    return direct + spread[None] * trial_wide
```

```python
import jax
import jax.numpy as jnp
from jax import lax
from jax.experimental import pallas as pl
from jax.experimental.pallas import tpu as pltpu
from jax.sharding import PartitionSpec as P

MESH = pl.DeviceIdType.MESH
F32, BF16 = jnp.float32, jnp.bfloat16

X, YH, YL, Z = 4, 2, 2, 8
NK, NO, NV = 8, 256, 512
CH = 4
KC = NK // CH
LINES = X * YL
ROWS = NO // LINES
OWN = NO // (LINES * Z)
AUX = 32
W = 128
MB = 2048


def nt(a, b):
    return lax.dot_general(a, b, (((1,), (1,)), ((), ())), preferred_element_type=F32)


def kernel(
    trial, hole_hbm, elec_hbm, out,
    elec, hole, hole_t, rz, line, full, half, acc, part, got, part2, got2,
    load_sem, zs, zr, ps, pr, cs, cr, s1, r1, s2, r2,
):
    f, c = lax.axis_index("fit"), lax.axis_index("col")
    x, yl, z = f // (YL * Z), (f // Z) % YL, f % Z
    yh, core = c // 2, c % 2
    ln = f // Z
    y = yh * YL + yl
    q = x * 4 + y

    def at_z(off):
        return (ln * Z + (z + off) % Z, c)

    def at_plane(off):
        q2 = (q + off) % 16
        x2, y2 = q2 // 4, q2 % 4
        return ((x2 * YL + y2 % YL) * Z + z, (y2 // YL) * 2 + core)

    def at_line(off):
        return (((ln + off) % LINES) * Z + z, c)

    partner = (f, yh * 2 + (1 - core))

    def load_hole():
        return pltpu.make_async_copy(hole_hbm, hole, load_sem.at[0])

    def load_elec():
        return pltpu.make_async_copy(elec_hbm, elec, load_sem.at[1])

    load_hole().start()
    load_elec().start()

    barrier = pltpu.get_barrier_semaphore()

    @pl.loop(1, Z)
    def _(off):
        pl.semaphore_signal(barrier, inc=1, device_id=at_z(off), device_id_type=MESH)

    @pl.loop(1, 16)
    def _(off):
        pl.semaphore_signal(barrier, inc=1, device_id=at_plane(off), device_id_type=MESH)

    pl.semaphore_signal(barrier, inc=1, device_id=partner, device_id_type=MESH)
    pl.semaphore_wait(barrier, Z - 1 + 15 + 1)

    def z_copy(off):
        return pltpu.make_async_remote_copy(
            src_ref=trial, dst_ref=rz.at[z], send_sem=zs.at[off], recv_sem=zr.at[off],
            device_id=at_z(off), device_id_type=MESH,
        )

    @pl.loop(1, Z)
    def _(off):
        z_copy(off).start()

    rz[z] = trial[...]
    load_hole().wait()

    @pl.loop(0, AUX)
    def _(p):
        hole_t[pl.ds(pl.multiple_of(p * NO, NO), NO), :] = hole[p].T

    @pl.loop(1, Z)
    def _(off):
        z_copy(off).wait_recv()

    for zz in range(Z):
        for k in range(NK):
            line[k, zz * OWN : (zz + 1) * OWN, :] = rz[zz, k].astype(F32)
    mine = pl.ds(pl.multiple_of(ln * ROWS, ROWS), ROWS)
    full[c, :, mine, :] = line[...].astype(BF16)

    def plane_copy(ch, off):
        here = full.at[c, pl.ds(ch * KC, KC), mine, :]
        return pltpu.make_async_remote_copy(
            src_ref=here, dst_ref=here, send_sem=ps.at[ch, off], recv_sem=pr.at[ch, off],
            device_id=at_plane(off), device_id_type=MESH,
        )

    for ch in range(CH):
        @pl.loop(1, 16)
        def _(off):
            plane_copy(ch, off).start()

    def core_copy(ch, h):
        here = full.at[2 * h + core, pl.ds(ch * KC, KC)]
        return pltpu.make_async_remote_copy(
            src_ref=here, dst_ref=here, send_sem=cs.at[ch, h], recv_sem=cr.at[ch, h],
            device_id=partner, device_id_type=MESH,
        )

    def hand_over(ch):
        @pl.loop(1, 16)
        def _(off):
            plane_copy(ch, off).wait_recv()

        for h in range(2):
            core_copy(ch, h).start()

    def sum_copy(ch, off):
        there = (ln + off) % LINES
        return pltpu.make_async_remote_copy(
            src_ref=part.at[ch, pl.ds(pl.multiple_of(there * ROWS, ROWS), ROWS), :],
            dst_ref=got.at[ch, ln], send_sem=s1.at[ch, off], recv_sem=r1.at[ch, off],
            device_id=at_line(off), device_id_type=MESH,
        )

    def sum2_copy(ch, off):
        return pltpu.make_async_remote_copy(
            src_ref=part2.at[ch, (z + off) % Z], dst_ref=got2.at[ch, z],
            send_sem=s2.at[ch, off], recv_sem=r2.at[ch, off],
            device_id=at_z(off), device_id_type=MESH,
        )

    def first_sum(ch):
        @pl.loop(1, LINES)
        def _(off):
            sum_copy(ch, off).wait_recv()

        total = got[ch, 0].astype(F32)
        for n in range(1, LINES):
            total = total + got[ch, n].astype(F32)
        for zz in range(Z):
            part2[ch, zz] = total[zz * OWN : (zz + 1) * OWN, :]
        got2[ch, z] = part2[ch, z]

        @pl.loop(1, Z)
        def _(off):
            sum2_copy(ch, off).start()

    def second_sum(ch):
        @pl.loop(1, Z)
        def _(off):
            sum2_copy(ch, off).wait_recv()

        total = got2[ch, 0]
        for n in range(1, Z):
            total = total + got2[ch, n]
        for kk in range(KC):
            out[ch * KC + kk] = total[:, kk * W : (kk + 1) * W]

    load_elec().wait()
    hand_over(0)
    for ch in range(CH):
        for h in range(2):
            core_copy(ch, h).wait_recv()

        for kk in range(KC):
            @pl.loop(0, AUX * W // MB)
            def _(m):
                left = elec[pl.ds(pl.multiple_of(m * MB, MB), MB), :]
                right = jnp.concatenate([full[b, ch * KC + kk] for b in range(4)], axis=1)
                made = nt(left, right)
                for p in range(MB // W):
                    at = pl.multiple_of(m * (MB // W * NO) + p * NO, NO)
                    half[kk * W : (kk + 1) * W, pl.ds(at, NO)] = made[p * W : (p + 1) * W].astype(BF16)

        if ch + 1 < CH:
            hand_over(ch + 1)
        if ch >= 1:
            first_sum(ch - 1)

        acc[...] = jnp.dot(half[...], hole_t[...], preferred_element_type=F32)
        part[ch] = acc[...].T.astype(BF16)
        got[ch, ln] = part[ch, mine, :]

        @pl.loop(1, LINES)
        def _(off):
            sum_copy(ch, off).start()

        if ch >= 2:
            second_sum(ch - 2)

    first_sum(CH - 1)
    second_sum(CH - 2)
    second_sum(CH - 1)

    @pl.loop(1, Z)
    def _(off):
        z_copy(off).wait_send()

    for ch in range(CH):
        @pl.loop(1, 16)
        def _(off):
            plane_copy(ch, off).wait_send()

        for h in range(2):
            core_copy(ch, h).wait_send()

        @pl.loop(1, LINES)
        def _(off):
            sum_copy(ch, off).wait_send()

        @pl.loop(1, Z)
        def _(off):
            sum2_copy(ch, off).wait_send()


def local(trial, hole_factor, elec_factor, hole_energy, elec_energy):
    vmem, hbm = pl.BlockSpec(memory_space=pltpu.VMEM), pl.BlockSpec(memory_space=pl.ANY)
    dma = pltpu.SemaphoreType.DMA
    direct = pl.pallas_call(
        kernel,
        out_shape=jax.ShapeDtypeStruct((NK, OWN, W), F32),
        in_specs=[vmem, hbm, hbm],
        out_specs=vmem,
        scratch_shapes=[
            pltpu.VMEM((AUX * W, NV), BF16),
            pltpu.VMEM((AUX, NO, NO), BF16),
            pltpu.VMEM((AUX * NO, NO), BF16),
            pltpu.VMEM((Z, NK, OWN, W), BF16),
            pltpu.VMEM((NK, ROWS, W), F32),
            pltpu.VMEM((4, NK, NO, W), BF16),
            pltpu.VMEM((KC * W, AUX * NO), BF16),
            pltpu.VMEM((KC * W, NO), F32),
            pltpu.VMEM((CH, NO, KC * W), BF16),
            pltpu.VMEM((CH, LINES, ROWS, KC * W), BF16),
            pltpu.VMEM((CH, Z, OWN, KC * W), F32),
            pltpu.VMEM((CH, Z, OWN, KC * W), F32),
            dma((2,)),
            dma((Z,)), dma((Z,)),
            dma((CH, 16)), dma((CH, 16)),
            dma((CH, 2)), dma((CH, 2)),
            dma((CH, LINES)), dma((CH, LINES)),
            dma((CH, Z)), dma((CH, Z)),
        ],
        compiler_params=pltpu.CompilerParams(
            collective_id=0, has_side_effects=True, vmem_limit_bytes=60 * 1024 * 1024
        ),
        name="bse_direct",
    )(trial, hole_factor, elec_factor.reshape(AUX * W, NV))
    spread = elec_energy[None, :] - hole_energy[:, None]
    return direct + spread[None] * trial.astype(F32)


def solution(mesh):
    in_specs = (
        P(None, "fit", "col"),
        P("fit", None, None),
        P("fit", "col", None),
        P("fit"),
        P("col"),
    )
    out_specs = P(None, "fit", "col")
    return jax.shard_map(local, mesh=mesh, in_specs=in_specs, out_specs=out_specs, check_vma=False)
```

```python
import jax
import jax.numpy as jnp
from jax import lax
from jax.experimental import pallas as pl
from jax.experimental.pallas import tpu as pltpu
from jax.sharding import PartitionSpec as P

MESH = pl.DeviceIdType.MESH
F32, BF16 = jnp.float32, jnp.bfloat16

X, YH, YL, Z = 4, 2, 2, 8
PLANE = X * YH * YL
NK, NO, NV = 8, 256, 512
CH = 4
KC = NK // CH
LINES = X * YL
ROWS = NO // LINES
OWN = NO // (LINES * Z)
AUX = 32
W = 128
MB = 2048
LAG, LAG2 = 2, 4


def nt(a, b):
    return lax.dot_general(a, b, (((1,), (1,)), ((), ())), preferred_element_type=F32)


def kernel(
    trial, hole_hbm, elec_hbm, hole_e, elec_e, out,
    elec, hole, hole_t, rz, line, full, half, acc, part, got, part2, got2,
    load_sem, zs, zr, ps, pr, cs, cr, s1, r1, s2, r2,
):
    f, c = lax.axis_index("fit"), lax.axis_index("col")
    ln, z = lax.div(f, Z), lax.rem(f, Z)
    x, yl = lax.div(ln, YL), lax.rem(ln, YL)
    yh, core = lax.div(c, 2), lax.rem(c, 2)
    q = x * 4 + yh * YL + yl

    def plane_of(off):
        q2 = lax.rem(q + off, PLANE)
        x2, y2 = lax.div(q2, 4), lax.rem(q2, 4)
        return (x2 * YL + lax.rem(y2, YL)) * Z + z, lax.div(y2, YL) * 2 + core

    z_at = [lax.rem(z + o, Z) for o in range(Z)]
    line_at = [lax.rem(ln + o, LINES) for o in range(LINES)]
    z_peer = [(ln * Z + z_at[o], c) for o in range(Z)]
    line_peer = [(line_at[o] * Z + z, c) for o in range(LINES)]
    plane_peer = [plane_of(o) for o in range(PLANE)]
    partner = (f, yh * 2 + (1 - core))
    mine = pl.ds(pl.multiple_of(ln * ROWS, ROWS), ROWS)

    def load(n, src, dst):
        return pltpu.make_async_copy(src, dst, load_sem.at[n])

    load_trial = load(0, trial, rz.at[z])
    load_hole = load(1, hole_hbm, hole)
    load_elec = load(2, elec_hbm, elec)
    load_trial.start()

    barrier = pltpu.get_barrier_semaphore()
    for peer in z_peer[1:] + plane_peer[1:] + [partner]:
        pl.semaphore_signal(barrier, inc=1, device_id=peer, device_id_type=MESH)
    load_hole.start()
    load_elec.start()
    load_trial.wait()
    pl.semaphore_wait(barrier, Z - 1 + PLANE - 1 + 1)

    def remote(src, dst, send, recv, peer):
        return pltpu.make_async_remote_copy(
            src_ref=src, dst_ref=dst, send_sem=send, recv_sem=recv, device_id=peer, device_id_type=MESH
        )

    def arrived(ref, sem):
        pltpu.make_async_copy(ref, ref, sem).wait()

    def send_line(n):
        here = rz.at[z, :KC] if n == 0 else rz.at[z, KC:]
        for off in range(1, Z):
            remote(here, here, zs.at[n], zr.at[n], z_peer[off]).start()

    def line_arrived(n):
        ks = range(KC) if n == 0 else range(KC, NK)
        arrived(rz.at[: Z - 1, ks.start : ks.stop], zr.at[n])
        for zz in range(Z):
            for k in ks:
                line[k, zz * OWN : (zz + 1) * OWN, :] = rz[zz, k].astype(F32)
        full[c, ks.start : ks.stop, mine, :] = line[ks.start : ks.stop].astype(BF16)

    send_line(0)
    load_hole.wait()

    @pl.loop(0, AUX)
    def _(p):
        hole_t[pl.ds(pl.multiple_of(p * NO, NO), NO), :] = hole[p].T

    send_line(1)

    def spread(ch):
        here = full.at[c, pl.ds(ch * KC, KC), mine, :]
        for off in range(1, PLANE):
            remote(here, here, ps.at[ch], pr.at[ch], plane_peer[off]).start()

    def spread_done(ch):
        arrived(full.at[0, : KC * 2, : ROWS * (PLANE - 1) // 2], ps.at[ch])

    def hand_over(ch):
        arrived(full.at[0, : KC * 2, : ROWS * (PLANE - 1) // 2], pr.at[ch])
        for h in range(2):
            here = full.at[2 * h + core, pl.ds(ch * KC, KC)]
            remote(here, here, cs.at[ch], cr.at[ch], partner).start()

    def send_sums(ch):
        for off in range(1, LINES):
            rows = pl.ds(pl.multiple_of(line_at[off] * ROWS, ROWS), ROWS)
            remote(part.at[ch, rows, :], got.at[ch, ln], s1, r1.at[ch], line_peer[off]).start()

    def first_sum(ch):
        arrived(got.at[ch, : LINES - 1], r1.at[ch])
        total = got[ch, 0].astype(F32)
        for n in range(1, LINES):
            total = total + got[ch, n].astype(F32)
        for zz in range(Z):
            part2[ch, zz] = total[zz * OWN : (zz + 1) * OWN, :]
        got2[ch, z] = part2[ch, z]
        for off in range(1, Z):
            remote(part2.at[ch, z_at[off]], got2.at[ch, z], s2, r2.at[ch], z_peer[off]).start()

    def second_sum(ch):
        arrived(got2.at[ch, : Z - 1], r2.at[ch])
        total = got2[ch, 0]
        for n in range(1, Z):
            total = total + got2[ch, n]
        for kk in range(KC):
            k = ch * KC + kk
            out[k] = total[:, kk * W : (kk + 1) * W] + gap * rz[z, k].astype(F32)

    gap = jnp.concatenate([elec_e[...] - hole_e[i] for i in range(OWN)], axis=0)
    line_arrived(0)
    spread(0)
    line_arrived(1)
    load_elec.wait()
    spread_done(0)
    spread(1)
    hand_over(0)
    for ch in range(CH):
        arrived(full.at[:2, :KC], cr.at[ch])

        @pl.loop(0, AUX * W // MB)
        def _(m):
            left = elec[pl.ds(pl.multiple_of(m * MB, MB), MB), :]
            right = jnp.concatenate(
                [
                    jnp.concatenate([full[b, ch * KC + kk] for b in range(4)], axis=1)
                    for kk in range(KC)
                ],
                axis=0,
            )
            made = nt(left, right)
            for p in range(MB // W):
                at = pl.multiple_of(m * (MB // W * NO) + p * NO, NO)
                for kk in range(KC):
                    half[kk * W : (kk + 1) * W, pl.ds(at, NO)] = made[
                        p * W : (p + 1) * W, kk * NO : (kk + 1) * NO
                    ].astype(BF16)

            if ch + 2 < CH:
                @pl.when(m == 0)
                def _():
                    spread_done(ch + 1)
                    spread(ch + 2)

        if ch + 1 < CH:
            hand_over(ch + 1)
        if ch >= LAG:
            first_sum(ch - LAG)

        acc[...] = jnp.dot(half[...], hole_t[...], preferred_element_type=F32)
        part[ch] = acc[...].T.astype(BF16)
        got[ch, ln] = part[ch, mine, :]
        send_sums(ch)

        if ch >= LAG2:
            second_sum(ch - LAG2)

    for ch in range(CH - LAG, CH):
        first_sum(ch)
    for ch in range(CH - LAG2, CH):
        second_sum(ch)

    arrived(rz.at[: Z - 1, :KC], zs.at[0])
    arrived(rz.at[: Z - 1, KC:], zs.at[1])
    spread_done(CH - 1)
    for ch in range(CH):
        arrived(full.at[:2, :KC], cs.at[ch])
    arrived(got.at[:, : LINES - 1], s1)
    arrived(got2.at[:, : Z - 1], s2)


def local(trial, hole_factor, elec_factor, hole_energy, elec_energy):
    vmem, hbm = pl.BlockSpec(memory_space=pltpu.VMEM), pl.BlockSpec(memory_space=pl.ANY)
    dma = pltpu.SemaphoreType.DMA
    return pl.pallas_call(
        kernel,
        out_shape=jax.ShapeDtypeStruct((NK, OWN, W), F32),
        in_specs=[hbm, hbm, hbm, pl.BlockSpec(memory_space=pltpu.SMEM), vmem],
        out_specs=vmem,
        scratch_shapes=[
            pltpu.VMEM((AUX * W, NV), BF16),
            pltpu.VMEM((AUX, NO, NO), BF16),
            pltpu.VMEM((AUX * NO, NO), BF16),
            pltpu.VMEM((Z, NK, OWN, W), BF16),
            pltpu.VMEM((NK, ROWS, W), F32),
            pltpu.VMEM((4, NK, NO, W), BF16),
            pltpu.VMEM((KC * W, AUX * NO), BF16),
            pltpu.VMEM((KC * W, NO), F32),
            pltpu.VMEM((CH, NO, KC * W), BF16),
            pltpu.VMEM((CH, LINES, ROWS, KC * W), BF16),
            pltpu.VMEM((CH, Z, OWN, KC * W), F32),
            pltpu.VMEM((CH, Z, OWN, KC * W), F32),
            dma((3,)),
            dma((2,)), dma((2,)),
            dma((CH,)), dma((CH,)),
            dma((CH,)), dma((CH,)),
            dma, dma((CH,)),
            dma, dma((CH,)),
        ],
        compiler_params=pltpu.CompilerParams(
            collective_id=0, has_side_effects=True, vmem_limit_bytes=60 * 1024 * 1024
        ),
        name="bse_direct",
    )(
        trial, hole_factor, elec_factor.reshape(AUX * W, NV),
        hole_energy, elec_energy.reshape(1, W),
    )


def solution(mesh):
    in_specs = (
        P(None, "fit", "col"),
        P("fit", None, None),
        P("fit", "col", None),
        P("fit"),
        P("col"),
    )
    out_specs = P(None, "fit", "col")
    return jax.shard_map(local, mesh=mesh, in_specs=in_specs, out_specs=out_specs, check_vma=False)
```

```python
import jax
import jax.numpy as jnp
from jax import lax
from jax.experimental import pallas as pl
from jax.experimental.pallas import tpu as pltpu
from jax.sharding import PartitionSpec as P

MESH = pl.DeviceIdType.MESH
F32, BF16 = jnp.float32, jnp.bfloat16

X, YH, YL, Z = 4, 2, 2, 8
PLANE = X * YH * YL
NK, NO, NV = 8, 256, 512
CH = 4
KC = NK // CH
LINES = X * YL
ROWS = NO // LINES
OWN = NO // (LINES * Z)
AUX = 32
W = 128
MB = 2048
LAG, LAG2 = 2, 4


def nt(a, b):
    return lax.dot_general(a, b, (((1,), (1,)), ((), ())), preferred_element_type=F32)


def kernel(
    trial, hole_hbm, elec_hbm, hole_e_hbm, elec_e_hbm, out,
    hole_e, elec_e, elec, hole, hole_t, rz, line, full, half, acc, part, got, part2, got2,
    load_sem, zs, zr, ps, pr, cs, cr, s1, r1, s2, r2,
):
    f, c = lax.axis_index("fit"), lax.axis_index("col")
    ln, z = lax.div(f, Z), lax.rem(f, Z)
    x, yl = lax.div(ln, YL), lax.rem(ln, YL)
    yh, core = lax.div(c, 2), lax.rem(c, 2)
    q = x * 4 + yh * YL + yl

    def plane_of(off):
        q2 = lax.rem(q + off, PLANE)
        x2, y2 = lax.div(q2, 4), lax.rem(q2, 4)
        return (x2 * YL + lax.rem(y2, YL)) * Z + z, lax.div(y2, YL) * 2 + core

    z_at = [lax.rem(z + o, Z) for o in range(Z)]
    line_at = [lax.rem(ln + o, LINES) for o in range(LINES)]
    z_peer = [(ln * Z + z_at[o], c) for o in range(Z)]
    line_peer = [(line_at[o] * Z + z, c) for o in range(LINES)]
    plane_peer = [plane_of(o) for o in range(PLANE)]
    partner = (f, yh * 2 + (1 - core))
    mine = pl.ds(pl.multiple_of(ln * ROWS, ROWS), ROWS)

    def load(n, src, dst):
        return pltpu.make_async_copy(src, dst, load_sem.at[n])

    load_trial = load(0, trial, rz.at[z])
    load_hole = load(1, hole_hbm, hole)
    load_elec = load(2, elec_hbm, elec)
    load_energies = [load(3, hole_e_hbm, hole_e), load(4, elec_e_hbm, elec_e)]
    load_trial.start()

    barrier = pltpu.get_barrier_semaphore()
    for peer in z_peer[1:] + plane_peer[1:] + [partner]:
        pl.semaphore_signal(barrier, inc=1, device_id=peer, device_id_type=MESH)
    load_hole.start()
    load_elec.start()
    for one in load_energies:
        one.start()
    load_trial.wait()
    pl.semaphore_wait(barrier, Z - 1 + PLANE - 1 + 1)

    def remote(src, dst, send, recv, peer):
        return pltpu.make_async_remote_copy(
            src_ref=src, dst_ref=dst, send_sem=send, recv_sem=recv, device_id=peer, device_id_type=MESH
        )

    def arrived(ref, sem):
        pltpu.make_async_copy(ref, ref, sem).wait()

    def send_line(n):
        here = rz.at[z, :KC] if n == 0 else rz.at[z, KC:]
        for off in range(1, Z):
            remote(here, here, zs.at[n], zr.at[n], z_peer[off]).start()

    def line_arrived(n):
        ks = range(KC) if n == 0 else range(KC, NK)
        arrived(rz.at[: Z - 1, ks.start : ks.stop], zr.at[n])
        for zz in range(Z):
            for k in ks:
                line[k, zz * OWN : (zz + 1) * OWN, :] = rz[zz, k].astype(F32)
        full[c, ks.start : ks.stop, mine, :] = line[ks.start : ks.stop].astype(BF16)

    send_line(0)
    load_hole.wait()

    @pl.loop(0, AUX)
    def _(p):
        hole_t[pl.ds(pl.multiple_of(p * NO, NO), NO), :] = hole[p].T

    send_line(1)

    def spread(ch):
        here = full.at[c, pl.ds(ch * KC, KC), mine, :]
        for off in range(1, PLANE):
            remote(here, here, ps.at[ch], pr.at[ch], plane_peer[off]).start()

    def spread_done(ch):
        arrived(full.at[0, : KC * 2, : ROWS * (PLANE - 1) // 2], ps.at[ch])

    def hand_over(ch):
        arrived(full.at[0, : KC * 2, : ROWS * (PLANE - 1) // 2], pr.at[ch])
        for h in range(2):
            here = full.at[2 * h + core, pl.ds(ch * KC, KC)]
            remote(here, here, cs.at[ch], cr.at[ch], partner).start()

    def send_sums(ch):
        for off in range(1, LINES):
            rows = pl.ds(pl.multiple_of(line_at[off] * ROWS, ROWS), ROWS)
            remote(part.at[ch, rows, :], got.at[ch, ln], s1, r1.at[ch], line_peer[off]).start()

    def first_sum(ch):
        arrived(got.at[ch, : LINES - 1], r1.at[ch])
        total = got[ch, 0].astype(F32)
        for n in range(1, LINES):
            total = total + got[ch, n].astype(F32)
        for zz in range(Z):
            part2[ch, zz] = total[zz * OWN : (zz + 1) * OWN, :]
        got2[ch, z] = part2[ch, z]
        for off in range(1, Z):
            remote(part2.at[ch, z_at[off]], got2.at[ch, z], s2, r2.at[ch], z_peer[off]).start()

    def second_sum(ch):
        arrived(got2.at[ch, : Z - 1], r2.at[ch])
        total = got2[ch, 0]
        for n in range(1, Z):
            total = total + got2[ch, n]
        for kk in range(KC):
            k = ch * KC + kk
            out[k] = total[:, kk * W : (kk + 1) * W] + gap * rz[z, k].astype(F32)

    for one in load_energies:
        one.wait()
    gap = jnp.concatenate([elec_e[...] - hole_e[i] for i in range(OWN)], axis=0)
    line_arrived(0)
    spread(0)
    line_arrived(1)
    load_elec.wait()
    spread_done(0)
    spread(1)
    spread(2)
    hand_over(0)
    for ch in range(CH):
        arrived(full.at[:2, :KC], cr.at[ch])

        @pl.loop(0, AUX * W // MB)
        def _(m):
            left = elec[pl.ds(pl.multiple_of(m * MB, MB), MB), :]
            right = jnp.concatenate(
                [
                    jnp.concatenate([full[b, ch * KC + kk] for b in range(4)], axis=1)
                    for kk in range(KC)
                ],
                axis=0,
            )
            made = nt(left, right)
            for p in range(MB // W):
                at = pl.multiple_of(m * (MB // W * NO) + p * NO, NO)
                for kk in range(KC):
                    half[kk * W : (kk + 1) * W, pl.ds(at, NO)] = made[
                        p * W : (p + 1) * W, kk * NO : (kk + 1) * NO
                    ].astype(BF16)

            if ch == 0:
                @pl.when(m == 0)
                def _():
                    spread_done(1)
                    spread(3)

        if ch + 1 < CH:
            hand_over(ch + 1)
        if ch >= LAG:
            first_sum(ch - LAG)

        acc[...] = jnp.dot(half[...], hole_t[...], preferred_element_type=F32)
        part[ch] = acc[...].T.astype(BF16)
        got[ch, ln] = part[ch, mine, :]
        send_sums(ch)

        if ch >= LAG2:
            second_sum(ch - LAG2)

    for ch in range(CH - LAG, CH):
        first_sum(ch)
    for ch in range(CH - LAG2, CH):
        second_sum(ch)

    arrived(rz.at[: Z - 1, :KC], zs.at[0])
    arrived(rz.at[: Z - 1, KC:], zs.at[1])
    spread_done(2)
    spread_done(3)
    for ch in range(CH):
        arrived(full.at[:2, :KC], cs.at[ch])
    arrived(got.at[:, : LINES - 1], s1)
    arrived(got2.at[:, : Z - 1], s2)


def local(trial, hole_factor, elec_factor, hole_energy, elec_energy):
    vmem, hbm = pl.BlockSpec(memory_space=pltpu.VMEM), pl.BlockSpec(memory_space=pltpu.HBM)
    dma = pltpu.SemaphoreType.DMA
    return pl.pallas_call(
        kernel,
        out_shape=jax.ShapeDtypeStruct((NK, OWN, W), F32),
        in_specs=[hbm] * 5,
        out_specs=vmem,
        scratch_shapes=[
            pltpu.SMEM((OWN,), F32),
            pltpu.VMEM((1, W), F32),
            pltpu.VMEM((AUX * W, NV), BF16),
            pltpu.VMEM((AUX, NO, NO), BF16),
            pltpu.VMEM((AUX * NO, NO), BF16),
            pltpu.VMEM((Z, NK, OWN, W), BF16),
            pltpu.VMEM((NK, ROWS, W), F32),
            pltpu.VMEM((4, NK, NO, W), BF16),
            pltpu.VMEM((KC * W, AUX * NO), BF16),
            pltpu.VMEM((KC * W, NO), F32),
            pltpu.VMEM((CH, NO, KC * W), BF16),
            pltpu.VMEM((CH, LINES, ROWS, KC * W), BF16),
            pltpu.VMEM((CH, Z, OWN, KC * W), F32),
            pltpu.VMEM((CH, Z, OWN, KC * W), F32),
            dma((5,)),
            dma((2,)), dma((2,)),
            dma((CH,)), dma((CH,)),
            dma((CH,)), dma((CH,)),
            dma, dma((CH,)),
            dma, dma((CH,)),
        ],
        compiler_params=pltpu.CompilerParams(
            collective_id=0, has_side_effects=True, vmem_limit_bytes=60 * 1024 * 1024
        ),
        name="bse_direct",
    )(
        trial, hole_factor, elec_factor.reshape(AUX * W, NV),
        hole_energy, elec_energy.reshape(1, W),
    )


def solution(mesh):
    in_specs = (
        P(None, "fit", "col"),
        P("fit", None, None),
        P("fit", "col", None),
        P("fit"),
        P("col"),
    )
    out_specs = P(None, "fit", "col")
    return jax.shard_map(local, mesh=mesh, in_specs=in_specs, out_specs=out_specs, check_vma=False)
```

```python
import jax
import jax.numpy as jnp
from jax import lax
from jax.experimental import pallas as pl
from jax.experimental.pallas import tpu as pltpu
from jax.sharding import PartitionSpec as P

MESH = pl.DeviceIdType.MESH
F32, BF16 = jnp.float32, jnp.bfloat16

X, YH, YL, Z = 4, 2, 2, 8
PLANE = X * YH * YL
NK, NO, NV = 8, 256, 512
CH = 4
KC = NK // CH
LINES = X * YL
ROWS = NO // LINES
OWN = NO // (LINES * Z)
AUX = 32
W = 128
MB = 2048
LAG, LAG2 = 2, 4


def nt(a, b):
    return lax.dot_general(a, b, (((1,), (1,)), ((), ())), preferred_element_type=F32)


def kernel(
    trial, hole_hbm, elec_hbm, hole_e_hbm, elec_e_hbm, out,
    hole_e, elec_e, elec, hole, hole_t, rz, line, full, half, acc, part, got, part2, got2,
    load_sem, zs, zr, ps, pr, cs, cr, s1, r1, s2, r2,
):
    f, c = lax.axis_index("fit"), lax.axis_index("col")
    ln, z = lax.div(f, Z), lax.rem(f, Z)
    x, yl = lax.div(ln, YL), lax.rem(ln, YL)
    yh, core = lax.div(c, 2), lax.rem(c, 2)
    q = x * 4 + yh * YL + yl

    def plane_of(off):
        q2 = lax.rem(q + off, PLANE)
        x2, y2 = lax.div(q2, 4), lax.rem(q2, 4)
        return (x2 * YL + lax.rem(y2, YL)) * Z + z, lax.div(y2, YL) * 2 + core

    z_at = [lax.rem(z + o, Z) for o in range(Z)]
    line_at = [lax.rem(ln + o, LINES) for o in range(LINES)]
    z_peer = [(ln * Z + z_at[o], c) for o in range(Z)]
    line_peer = [(line_at[o] * Z + z, c) for o in range(LINES)]
    plane_peer = [plane_of(o) for o in range(PLANE)]
    partner = (f, yh * 2 + (1 - core))
    mine = pl.ds(pl.multiple_of(ln * ROWS, ROWS), ROWS)

    def load(n, src, dst):
        return pltpu.make_async_copy(src, dst, load_sem.at[n])

    load_trial = load(0, trial, rz.at[z])
    load_hole = load(1, hole_hbm, hole)
    load_elec = load(2, elec_hbm, elec)
    load_energies = [load(3, hole_e_hbm, hole_e), load(4, elec_e_hbm, elec_e)]
    load_trial.start()

    barrier = pltpu.get_barrier_semaphore()
    for peer in z_peer[1:] + plane_peer[1:] + [partner]:
        pl.semaphore_signal(barrier, inc=1, device_id=peer, device_id_type=MESH)
    load_hole.start()
    load_elec.start()
    for one in load_energies:
        one.start()
    load_trial.wait()
    pl.semaphore_wait(barrier, Z - 1 + PLANE - 1 + 1)

    def remote(src, dst, send, recv, peer):
        return pltpu.make_async_remote_copy(
            src_ref=src, dst_ref=dst, send_sem=send, recv_sem=recv, device_id=peer, device_id_type=MESH
        )

    def arrived(ref, sem):
        pltpu.make_async_copy(ref, ref, sem).wait()

    def send_line(n):
        here = rz.at[z, :KC] if n == 0 else rz.at[z, KC:]
        for off in range(1, Z):
            remote(here, here, zs.at[n], zr.at[n], z_peer[off]).start()

    def line_arrived(n):
        ks = range(KC) if n == 0 else range(KC, NK)
        arrived(rz.at[: Z - 1, ks.start : ks.stop], zr.at[n])
        for zz in range(Z):
            for k in ks:
                line[k, zz * OWN : (zz + 1) * OWN, :] = rz[zz, k].astype(F32)
        full[c, ks.start : ks.stop, mine, :] = line[ks.start : ks.stop].astype(BF16)

    send_line(0)
    load_hole.wait()

    @pl.loop(0, AUX)
    def _(p):
        hole_t[pl.ds(pl.multiple_of(p * NO, NO), NO), :] = hole[p].T

    send_line(1)

    def spread(ch):
        here = full.at[c, pl.ds(ch * KC, KC), mine, :]
        for off in range(1, PLANE):
            remote(here, here, ps.at[ch], pr.at[ch], plane_peer[off]).start()

    def spread_done(ch):
        arrived(full.at[0, : KC * 2, : ROWS * (PLANE - 1) // 2], ps.at[ch])

    def hand_over(ch):
        arrived(full.at[0, : KC * 2, : ROWS * (PLANE - 1) // 2], pr.at[ch])
        for h in range(2):
            here = full.at[2 * h + core, pl.ds(ch * KC, KC)]
            remote(here, here, cs.at[ch], cr.at[ch], partner).start()

    def send_sums(ch):
        for off in range(1, LINES):
            rows = pl.ds(pl.multiple_of(line_at[off] * ROWS, ROWS), ROWS)
            remote(part.at[ch, rows, :], got.at[ch, ln], s1, r1.at[ch], line_peer[off]).start()

    def first_sum(ch):
        arrived(got.at[ch, : LINES - 1], r1.at[ch])
        total = got[ch, 0].astype(F32)
        for n in range(1, LINES):
            total = total + got[ch, n].astype(F32)
        for zz in range(Z):
            part2[ch, zz] = total[zz * OWN : (zz + 1) * OWN, :]
        got2[ch, z] = part2[ch, z]
        for off in range(1, Z):
            remote(part2.at[ch, z_at[off]], got2.at[ch, z], s2, r2.at[ch], z_peer[off]).start()

    def second_sum(ch):
        arrived(got2.at[ch, : Z - 1], r2.at[ch])
        total = got2[ch, 0]
        for n in range(1, Z):
            total = total + got2[ch, n]
        for kk in range(KC):
            k = ch * KC + kk
            out[k] = total[:, kk * W : (kk + 1) * W] + gap * rz[z, k].astype(F32)

    for one in load_energies:
        one.wait()
    gap = jnp.concatenate([elec_e[...] - hole_e[i] for i in range(OWN)], axis=0)
    line_arrived(0)
    spread(0)
    line_arrived(1)
    load_elec.wait()
    spread_done(0)
    spread(1)
    hand_over(0)
    spread(2)
    for ch in range(CH):
        arrived(full.at[:2, :KC], cr.at[ch])

        @pl.loop(0, AUX * W // MB)
        def _(m):
            left = elec[pl.ds(pl.multiple_of(m * MB, MB), MB), :]
            right = jnp.concatenate(
                [
                    jnp.concatenate([full[b, ch * KC + kk] for b in range(4)], axis=1)
                    for kk in range(KC)
                ],
                axis=0,
            )
            made = nt(left, right)
            for p in range(MB // W):
                at = pl.multiple_of(m * (MB // W * NO) + p * NO, NO)
                for kk in range(KC):
                    half[kk * W : (kk + 1) * W, pl.ds(at, NO)] = made[
                        p * W : (p + 1) * W, kk * NO : (kk + 1) * NO
                    ].astype(BF16)

            if ch == 0:
                @pl.when(m == 0)
                def _():
                    spread(3)

        if ch + 1 < CH:
            hand_over(ch + 1)
        if ch >= LAG:
            first_sum(ch - LAG)

        acc[...] = jnp.dot(half[...], hole_t[...], preferred_element_type=F32)
        part[ch] = acc[...].T.astype(BF16)
        got[ch, ln] = part[ch, mine, :]
        send_sums(ch)

        if ch >= LAG2:
            second_sum(ch - LAG2)

    for ch in range(CH - LAG, CH):
        first_sum(ch)
    for ch in range(CH - LAG2, CH):
        second_sum(ch)

    arrived(rz.at[: Z - 1, :KC], zs.at[0])
    arrived(rz.at[: Z - 1, KC:], zs.at[1])
    for ch in range(1, CH):
        spread_done(ch)
    for ch in range(CH):
        arrived(full.at[:2, :KC], cs.at[ch])
    arrived(got.at[:, : LINES - 1], s1)
    arrived(got2.at[:, : Z - 1], s2)


def local(trial, hole_factor, elec_factor, hole_energy, elec_energy):
    vmem, hbm = pl.BlockSpec(memory_space=pltpu.VMEM), pl.BlockSpec(memory_space=pltpu.HBM)
    dma = pltpu.SemaphoreType.DMA
    return pl.pallas_call(
        kernel,
        out_shape=jax.ShapeDtypeStruct((NK, OWN, W), F32),
        in_specs=[hbm] * 5,
        out_specs=vmem,
        scratch_shapes=[
            pltpu.SMEM((OWN,), F32),
            pltpu.VMEM((1, W), F32),
            pltpu.VMEM((AUX * W, NV), BF16),
            pltpu.VMEM((AUX, NO, NO), BF16),
            pltpu.VMEM((AUX * NO, NO), BF16),
            pltpu.VMEM((Z, NK, OWN, W), BF16),
            pltpu.VMEM((NK, ROWS, W), F32),
            pltpu.VMEM((4, NK, NO, W), BF16),
            pltpu.VMEM((KC * W, AUX * NO), BF16),
            pltpu.VMEM((KC * W, NO), F32),
            pltpu.VMEM((CH, NO, KC * W), BF16),
            pltpu.VMEM((CH, LINES, ROWS, KC * W), BF16),
            pltpu.VMEM((CH, Z, OWN, KC * W), F32),
            pltpu.VMEM((CH, Z, OWN, KC * W), F32),
            dma((5,)),
            dma((2,)), dma((2,)),
            dma((CH,)), dma((CH,)),
            dma((CH,)), dma((CH,)),
            dma, dma((CH,)),
            dma, dma((CH,)),
        ],
        compiler_params=pltpu.CompilerParams(
            collective_id=0, has_side_effects=True, vmem_limit_bytes=60 * 1024 * 1024
        ),
        name="bse_direct",
    )(
        trial, hole_factor, elec_factor.reshape(AUX * W, NV),
        hole_energy, elec_energy.reshape(1, W),
    )


def solution(mesh):
    in_specs = (
        P(None, "fit", "col"),
        P("fit", None, None),
        P("fit", "col", None),
        P("fit"),
        P("col"),
    )
    out_specs = P(None, "fit", "col")
    return jax.shard_map(local, mesh=mesh, in_specs=in_specs, out_specs=out_specs, check_vma=False)
```
